32 devices in a mesh: py: 8 (over z, x), px: 4 (over y, core).
Axes of the slice: x: 2, y: 2, z: 4, core: 2. Of those that a mesh axis runs over, the one named last changes fastest.
Arguments:
- density: float32 [256, 128, 128], P('py', 'px'), may hold values from 0.5 to 2
- conductance: float32 [256, 128, 128], P('py', 'px'), may hold values from 0.03 to 0.22
- source: float32 [256, 128, 128], P('py', 'px'), may hold values from -0.2 to 0.2
Outputs:
- anomaly: float32 [256, 128, 128], P('py', 'px')
- density_end: float32 [256, 128, 128], P('py', 'px')
The draws below stay inside these ranges and needn't reach their ends.
All inputs are finite; a program needn't handle non-finite values.
Results may differ from the reference program's by a relative error of at most 0.00002.
Values sent between devices are 32-bit elements; how exact they have to be, the bound alone decides.
A program may use at most 64 MiB of HBM per device.

```python
import jax
import jax.numpy as jnp
from jax import lax

GRID_Y = 256
GRID_X = 128
LEVELS = 128
STEPS = 6


def steps_of(rng, shape, cuts, least, high):
    loudness, own = 1.0, jax.random.fold_in(rng, 6)
    for dim, shards_of in cuts:
        steps = jnp.exp(jax.random.uniform(jax.random.fold_in(own, dim), (shards_of,), jnp.float32, least / len(cuts), high / len(cuts)))
        loudness = loudness * jnp.repeat(steps, shape[dim] // shards_of).reshape([-1 if axis == dim else 1 for axis in range(len(shape))])
    return loudness


def setup_inputs(seed: int = 0) -> dict:
    key_list = jax.random.split(jax.random.key(seed), 4)
    return {
        "density": jnp.clip(0.5 + 1.5 * jax.random.uniform(key_list[0], (GRID_Y, GRID_X, LEVELS), jnp.float32) ** steps_of(key_list[0], (GRID_Y, GRID_X, LEVELS), ((0, 8), (1, 4)), -0.2, 0.2), 0.5, 2.0),
        "conductance": jnp.clip(0.03 + 0.19 * jax.random.uniform(key_list[1], (GRID_Y, GRID_X, LEVELS), jnp.float32) ** steps_of(key_list[1], (GRID_Y, GRID_X, LEVELS), ((0, 8), (1, 4)), -0.2, 0.2), 0.03, 0.22),
        "source": jnp.clip(jax.random.uniform(key_list[2], (GRID_Y, GRID_X, LEVELS), jnp.float32, -0.2, 0.2) * steps_of(key_list[2], (GRID_Y, GRID_X, LEVELS), ((0, 8), (1, 4)), -0.4, 0.0), -0.2, 0.2),
    }


def strip_edges(values, dims):
    for dim in dims:
        values = lax.slice_in_dim(values, 1, values.shape[dim] - 1, axis=dim)
    return values

def neighbour(values, dim, start, dims):
    others = [other for other in dims if other != dim]
    values = strip_edges(values, others)
    return lax.slice_in_dim(values, start, start + values.shape[dim] - 2, axis=dim)

def one_step(padded, conductance, source):
    middle = strip_edges(padded, (0, 1))
    lower = [neighbour(padded, dim, 0, (0, 1)) for dim in (0, 1)]
    upper = [neighbour(padded, dim, 2, (0, 1)) for dim in (0, 1)]
    spread = lower[0] + upper[0] + lower[1] + upper[1] - 4.0 * middle
    return middle + conductance * spread + source

def reference(density, conductance, source):
    for step in range(STEPS):
        density = one_step(jnp.pad(density, ((1, 1), (1, 1), (0, 0)), mode='constant'), conductance, source)
    line_mean = lax.optimization_barrier(jnp.mean(density, axis=0, keepdims=True))
    centred = density - line_mean
    line_variance = lax.optimization_barrier(jnp.mean(centred * centred, axis=0, keepdims=True))
    anomaly = centred * lax.rsqrt(line_variance + 0.0001)
    return (anomaly, density)
```

```python
import functools

import jax
import jax.numpy as jnp
from jax import lax
from jax.experimental import pallas as pl
from jax.experimental.pallas import tpu as pltpu
from jax.sharding import PartitionSpec as P

ROUNDS = 2
DEEP = 3
PAD = 4
TOP = 2
DIRECTIONS = [(-1, 0), (1, 0), (-1, -1), (-1, 1), (1, -1), (1, 1), (0, -1), (0, 1)]
MESH = pl.DeviceIdType.MESH


def kernel(py, px, inner, field, conductance, source, density_out, mean_out, scale_out,
           padded, work, coefficients, ready, extra, stats, local_sem, send_sem, recv_sem,
           stat_send, stat_recv, present):
    rows, columns, levels = field.shape
    width = columns + 2 * PAD
    tall = rows + 2 * TOP
    my, mx = lax.axis_index("py"), lax.axis_index("px")

    def exists(dy, dx):
        here = jnp.bool_(True)
        if dy:
            here = here & ((my + dy >= 0) if dy < 0 else (my + dy < py))
        if dx:
            here = here & ((mx + dx >= 0) if dx < 0 else (mx + dx < px))
        return here

    own = pl.ds(PAD, columns)
    block = (pl.ds(TOP, rows), own)
    loads = []
    for i, (src, dst) in enumerate(
        [(field, padded.at[0]), (conductance, coefficients.at[0]), (source, coefficients.at[1])]
    ):
        loads.append(pltpu.make_async_copy(src, dst.at[block], local_sem.at[i]))
        loads[-1].start()

    barrier = pltpu.get_barrier_semaphore()
    expected = jnp.int32(0)
    for dy, dx in DIRECTIONS:
        there = exists(dy, dx)
        expected = expected + there.astype(jnp.int32)

        @pl.when(there)
        def _():
            pl.semaphore_signal(barrier, 1, device_id=(my + dy, mx + dx), device_id_type=MESH)

    holders = [padded.at[r] for r in range(ROUNDS)] + [coefficients.at[0], coefficients.at[1]]
    for side, dy in enumerate((-1, 1)):
        @pl.when(~exists(dy, 0))
        def _():
            for holder in holders[:-1]:
                start = 0 if dy < 0 else TOP + rows
                holder[pl.ds(start, TOP)] = jnp.zeros((TOP, width, levels), jnp.float32)
            for number in range(ROUNDS):
                extra[number, side] = jnp.zeros((2, width, levels), jnp.float32)
    for dx in (-1, 1):
        @pl.when(~exists(0, dx))
        def _():
            start = pl.ds(0 if dx < 0 else PAD + columns, PAD)
            for holder in holders:
                holder[:, start] = jnp.zeros((tall, PAD, levels), jnp.float32)
            for number in range(ROUNDS):
                for side in range(2):
                    extra[number, side, :, start] = jnp.zeros((2, PAD, levels), jnp.float32)

    pl.semaphore_wait(barrier, expected)

    edges = (TOP, TOP + rows - 1)
    beyond = (TOP - 1, TOP + rows)

    def remote(number, slot, direction, src, dst):
        d = DIRECTIONS.index(direction)
        return direction, pltpu.make_async_remote_copy(
            src_ref=src,
            dst_ref=dst,
            send_sem=send_sem.at[number, slot, d],
            recv_sem=recv_sem.at[number, slot, d],
            device_id=(my + direction[0], mx + direction[1]),
            device_id_type=MESH,
        )

    def start(copies):
        for (dy, dx), copy in copies:
            @pl.when(exists(dy, dx))
            def _():
                copy.start()

    def wait_recv(copies):
        for (dy, dx), copy in copies:
            @pl.when(exists(-dy, -dx))
            def _():
                copy.wait_recv()

    def wait_send(copies):
        for (dy, dx), copy in copies:
            @pl.when(exists(dy, dx))
            def _():
                copy.wait_send()

    def raw_rows(number, dy):
        side = 0 if dy < 0 else 1
        edge, far = edges[side], beyond[1 - side]
        second, far_second = edge - dy, far - dy
        out = [remote(number, 0, (dy, 0), padded.at[number, edge, own], padded.at[number, far, own])]
        if number == 0:
            out.append(remote(number, 1, (dy, 0), coefficients.at[0, edge, own], coefficients.at[0, far, own]))
            for slot, column in ((3, PAD), (4, PAD + columns - 1)):
                at = pl.ds(column, 1)
                out.append(remote(number, slot, (dy, 0), coefficients.at[0, second, at], coefficients.at[0, far_second, at]))
        for dx in (-1, 1):
            first, last = min(edge, second), min(far, far_second)
            from_ = PAD if dx < 0 else PAD + columns - 2
            to = PAD + columns if dx < 0 else PAD - 2
            out.append(remote(number, 0, (dy, dx), padded.at[number, pl.ds(first, 2), pl.ds(from_, 2)],
                              padded.at[number, pl.ds(last, 2), pl.ds(to, 2)]))
            if number == 0:
                from_ = PAD if dx < 0 else PAD + columns - 1
                to = PAD + columns if dx < 0 else PAD - 1
                out.append(remote(number, 1, (dy, dx), coefficients.at[0, edge, pl.ds(from_, 1)],
                                  coefficients.at[0, far, pl.ds(to, 1)]))
        return out

    def row_terms(number, dy):
        side = 0 if dy < 0 else 1
        out = [remote(number, 2, (dy, 0), ready.at[number, side], extra.at[number, 1 - side, :, own])]
        for dx in (-1, 1):
            from_ = 0 if dx < 0 else columns - 1
            to = PAD + columns if dx < 0 else PAD - 1
            out.append(remote(number, 2, (dy, dx), ready.at[number, side, 0, pl.ds(from_, 1)],
                              extra.at[number, 1 - side, 0, pl.ds(to, 1)]))
        return out

    def make_terms(number, dy):
        side = 0 if dy < 0 else 1
        edge = edges[side]
        second, third = edge - dy, edge - 2 * dy
        middle = padded[number, second, own]
        place = lax.broadcasted_iota(jnp.int32, (columns, levels), 0)
        before = jnp.where(place == 0, 0.0, pltpu.roll(middle, 1, 0))
        after = jnp.where(place == columns - 1, 0.0, pltpu.roll(middle, columns - 1, 0))
        spread = (padded[number, edge, own] + padded[number, third, own]) + (before + after) - 4.0 * middle
        later = middle + coefficients[0, second, own] * spread + coefficients[1, second, own]
        rate, gain = coefficients[0, edge, own], coefficients[1, edge, own]
        ready[number, side, 0] = rate * middle + gain
        ready[number, side, 1] = rate * later + gain

    def sideways(number, slot, first, count):
        out = []
        for dx in (-1, 1):
            arrays = [(padded.at[number], 3)]
            if number == 0:
                arrays += [(coefficients.at[0], 2), (coefficients.at[1], 2)]
            for a, (array, reach) in enumerate(arrays):
                from_ = PAD if dx < 0 else PAD + columns - reach
                to = PAD + columns if dx < 0 else PAD - reach
                out.append(remote(number, slot + a, (0, dx), array.at[pl.ds(first, count), pl.ds(from_, reach)],
                                  array.at[pl.ds(first, count), pl.ds(to, reach)]))
        return out

    flat_conductance = coefficients.at[0].reshape(tall * width, levels)
    flat_source = coefficients.at[1].reshape(tall * width, levels)

    def advance(old, first, count, column, wide, put, carry):
        flat = old.reshape(tall * width, levels)

        def row(i, state):
            above, middle, carry = state
            at = (first + i) * width + column
            below = flat[pl.ds(at + width, wide), :]
            sides = flat[pl.ds(at - 1, wide), :] + flat[pl.ds(at + 1, wide), :]
            spread = (above + below) + sides - 4.0 * middle
            later = middle + flat_conductance[pl.ds(at, wide), :] * spread + flat_source[pl.ds(at, wide), :]
            return middle, below, put(first - TOP + i, later, carry)

        at = first * width + column
        state = (flat[pl.ds(at - width, wide), :], flat[pl.ds(at, wide), :], carry)
        return lax.fori_loop(0, count, row, state, unroll=min(count, 4))[2]

    def advance_beyond(number, side, step, old, new):
        flat = old.reshape(tall * width, levels)
        at = beyond[side] * width
        inward = edges[side] * width
        middle = flat[pl.ds(at, width), :]
        sides = flat[pl.ds(at - 1, width), :] + flat[pl.ds(at + 1, width), :]
        spread = flat[pl.ds(inward, width), :] + sides - 4.0 * middle
        later = middle + flat_conductance[pl.ds(at, width), :] * spread + extra[number, side, step]
        new.reshape(tall * width, levels)[pl.ds(at, width), :] = later

    def mend(number, side):
        outward = 2 * side - 1
        far = beyond[side]
        for column, other in ((PAD, PAD - 1), (PAD + columns - 1, PAD + columns)):
            at, corner = pl.ds(column, 1), pl.ds(other, 1)
            extra[number, side, 1, at] = extra[number, side, 1, at] + (
                coefficients[0, far, at] * coefficients[0, far + outward, at]
            ) * padded[number, far + outward, corner]


    def announce(reach, index):
        for dy in (-reach, reach):
            @pl.when(exists(dy, 0))
            def _():
                pl.semaphore_signal(present.at[index], 1, device_id=(my + dy, mx), device_id_type=MESH)

    def hear(reach, index):
        count = exists(-reach, 0).astype(jnp.int32) + exists(reach, 0).astype(jnp.int32)
        pl.semaphore_wait(present.at[index], count)

    reaches = []
    while 2 ** (len(reaches) + 1) < py - 1:
        reaches.append(2 ** (len(reaches) + 1))

    for copy in loads:
        copy.wait()
    sent = []
    to_sides = [raw_rows(0, -1), raw_rows(0, 1)]
    for group in to_sides:
        start(group)
    for side, dy in enumerate((-1, 1)):
        make_terms(0, dy)
        terms = row_terms(0, dy)
        start(terms)
        to_sides[side] = to_sides[side] + terms
    across = sideways(0, 0, TOP, rows)
    start(across)

    total = jnp.zeros((columns, levels), jnp.float32)
    for number in range(ROUNDS):
        sent += across + to_sides[0] + to_sides[1]
        wait_recv(across)
        if number:
            if reaches:
                hear(reaches[0], 0)
            for index in range(1, min(2, len(reaches))):
                announce(reaches[index], index)
        next_sides, next_across = [], []
        for part in ("inside", "low", "high"):
            side = None if part == "inside" else (0 if part == "low" else 1)
            if side is not None:
                wait_recv(to_sides[1 - side])
                mend(number, side)
            old = padded.at[number]
            for step in range(DEEP):
                last = step == DEEP - 1
                if part == "inside":
                    first, count = TOP + step + 1, rows - 2 * (step + 1)
                elif part == "low":
                    first, count = TOP, step + 1
                else:
                    first, count = TOP + rows - step - 1, step + 1
                column, wide, new = 0, width, None
                if not last:
                    new = work.at[step]
                else:
                    column, wide = PAD, columns
                    if number < ROUNDS - 1:
                        new = padded.at[number + 1]

                def put(i, later, carry, new=new, column=column, wide=wide):
                    if new is None:
                        density_out[i] = later
                        return carry + later
                    new.reshape(tall * width, levels)[pl.ds((TOP + i) * width + column, wide), :] = later
                    return carry

                total = advance(old, first, count, column, wide, put, total)
                if side is not None and not last:
                    advance_beyond(number, side, step, old, new)
                old = new
            if number < ROUNDS - 1:
                if side is None:
                    some = sideways(number + 1, 0, TOP + DEEP, rows - 2 * DEEP)
                    start(some)
                    next_across += some
                else:
                    dy = 2 * side - 1
                    group = raw_rows(number + 1, dy)
                    start(group)
                    make_terms(number + 1, dy)
                    terms = row_terms(number + 1, dy)
                    start(terms)
                    next_sides.append(group + terms)
                    some = sideways(number + 1, 1 + side, TOP if side == 0 else TOP + rows - DEEP, DEEP)
                    start(some)
                    next_across += some
        if number == 0 and reaches:
            announce(reaches[0], 0)
        to_sides, across = next_sides, next_across

    local_mean = total * (1.0 / rows)

    def square(i, carry):
        away = density_out[i] - local_mean
        return carry + away * away

    squares = lax.fori_loop(0, rows, square, jnp.zeros((columns, levels), jnp.float32), unroll=4)
    stats[0, 0] = local_mean
    stats[0, 1] = squares
    for index in range(1, len(reaches)):
        hear(reaches[index], index)
        if index + 1 < len(reaches):
            announce(reaches[index + 1], index + 1)
    outer = py // inner
    far_first = sorted(
        ((do, di) for do in range(outer) for di in range(inner) if do or di),
        key=lambda place: -(min(place[0], outer - place[0]) + min(place[1], inner - place[1])),
    )
    sums = []
    for do, di in far_first:
        step = do * inner + di
        peer = lax.rem(my // inner + do, outer) * inner + lax.rem(lax.rem(my, inner) + di, inner)
        copy = pltpu.make_async_remote_copy(
            src_ref=stats.at[0],
            dst_ref=stats.at[step],
            send_sem=stat_send.at[step],
            recv_sem=stat_recv.at[step],
            device_id=(peer, mx),
            device_id_type=MESH,
        )
        copy.start()
        sums.append(copy)
    wait_send(sent)
    for copy in sums:
        copy.wait_recv()
    mean = stats[0, 0]
    for step in range(1, py):
        mean = mean + stats[step, 0]
    mean = mean * (1.0 / py)
    inside = stats[0, 1]
    between = (stats[0, 0] - mean) * (stats[0, 0] - mean)
    for step in range(1, py):
        inside = inside + stats[step, 1]
        between = between + (stats[step, 0] - mean) * (stats[step, 0] - mean)
    variance = inside * (1.0 / (rows * py)) + between * (1.0 / py)
    mean_out[...] = mean
    scale_out[...] = lax.rsqrt(variance + 0.0001)
    for copy in sums:
        copy.wait_send()

CHUNKS = 2


def finish(density, mean, scale, anomaly_out, density_out, anomaly, sem):
    rows = density.shape[0]
    whole = pltpu.make_async_copy(density, density_out, sem.at[CHUNKS])
    whole.start()
    part = rows // CHUNKS
    copies = []
    for chunk in range(CHUNKS):
        for i in range(chunk * part, (chunk + 1) * part):
            anomaly[i] = (density[i] - mean[...]) * scale[...]
        own = pl.ds(chunk * part, part)
        copies.append(pltpu.make_async_copy(anomaly.at[own], anomaly_out.at[own], sem.at[chunk]))
        copies[-1].start()
    for copy in copies:
        copy.wait()
    whole.wait()


def per_device(py, px, inner, density, conductance, source):
    rows, columns, levels = density.shape
    tall, width = rows + 2 * TOP, columns + 2 * PAD
    vmem = pl.BlockSpec(memory_space=pltpu.VMEM)
    line = jax.ShapeDtypeStruct((columns, levels), jnp.float32)
    density, conductance, source = (pltpu.with_memory_space_constraint(x, pltpu.HBM) for x in (density, conductance, source))
    density, mean, scale = pl.pallas_call(
        functools.partial(kernel, py, px, inner),
        out_shape=[jax.ShapeDtypeStruct(density.shape, jnp.float32), line, line],
        in_specs=[pl.BlockSpec(memory_space=pltpu.HBM)] * 3,
        out_specs=[vmem] * 3,
        scratch_shapes=[
            pltpu.VMEM((ROUNDS, tall, width, levels), jnp.float32),
            pltpu.VMEM((DEEP - 1, tall, width, levels), jnp.float32),
            pltpu.VMEM((2, tall, width, levels), jnp.float32),
            pltpu.VMEM((ROUNDS, 2, 2, columns, levels), jnp.float32),
            pltpu.VMEM((ROUNDS, 2, 2, width, levels), jnp.float32),
            pltpu.VMEM((py, 2, columns, levels), jnp.float32),
            pltpu.SemaphoreType.DMA((3,)),
            pltpu.SemaphoreType.DMA((ROUNDS, 5, len(DIRECTIONS))),
            pltpu.SemaphoreType.DMA((ROUNDS, 5, len(DIRECTIONS))),
            pltpu.SemaphoreType.DMA((py,)),
            pltpu.SemaphoreType.DMA((py,)),
            pltpu.SemaphoreType.REGULAR((8,)),
        ],
        compiler_params=pltpu.CompilerParams(collective_id=0, has_side_effects=True, vmem_limit_bytes=10*2**20),
    )(density, conductance, source)
    return pl.pallas_call(
        finish,
        out_shape=[jax.ShapeDtypeStruct(density.shape, jnp.float32)] * 2,
        in_specs=[vmem] * 3,
        out_specs=[pl.BlockSpec(memory_space=pltpu.HBM)] * 2,
        scratch_shapes=[pltpu.VMEM(density.shape, jnp.float32), pltpu.SemaphoreType.DMA((CHUNKS + 1,))],
        compiler_params=pltpu.CompilerParams(vmem_limit_bytes=4 * 2**20),
    )(density, mean, scale)


def solution(mesh):
    spec = P("py", "px", None)
    line = mesh.devices.reshape(mesh.shape["py"], -1)[:, 0] if mesh.axis_names[0] == "py" else []
    places = [getattr(device, "coords", (0, 0, 0))[2] for device in line]
    inner = max(1, places.count(places[0])) if places else 1
    return jax.shard_map(
        functools.partial(per_device, mesh.shape["py"], mesh.shape["px"], inner),
        mesh=mesh, in_specs=(spec,) * 3, out_specs=(spec,) * 2, check_vma=False,
    )
```

```python
import functools

import jax
import jax.numpy as jnp
from jax import lax
from jax.experimental import pallas as pl
from jax.experimental.pallas import tpu as pltpu
from jax.sharding import PartitionSpec as P

ROUNDS = 2
DEEP = 3
PAD = 4
TOP = 2
DIRECTIONS = [(-1, 0), (1, 0), (-1, -1), (-1, 1), (1, -1), (1, 1), (0, -1), (0, 1)]
MESH = pl.DeviceIdType.MESH
FIELD = (0, 3)
RATE, GAIN = 1, 2
CORNER = (5, 4)


def reaches_of(py):
    known, reaches = 1, []
    while known < py - 1:
        reaches.append(known)
        known *= 2
    return reaches


def parcel(number, columns):
    return (4 if number == 0 else 3) * columns + (2 if number == 0 else 0)


def kernel(py, px, inner, field, conductance, source, density_out, mean_out, scale_out,
           arrays, work, extra, parcel_out, parcel_in, corner_out, corner_in, stats,
           load_sem, send_sem, side_sem, across_sem, stat_sem, present):
    rows, columns, levels = field.shape
    width = columns + 2 * PAD
    tall = rows + 2 * TOP
    my, mx = lax.axis_index("py"), lax.axis_index("px")
    reaches = reaches_of(py)

    def exists(dy, dx):
        here = jnp.bool_(True)
        if dy:
            here = here & ((my + dy >= 0) if dy < 0 else (my + dy < py))
        if dx:
            here = here & ((mx + dx >= 0) if dx < 0 else (mx + dx < px))
        return here

    own = pl.ds(PAD, columns)
    middle_rows = rows - 2 * DEEP
    inputs = (field, conductance, source)
    for first, count, group in ((0, DEEP, 0), (rows - DEEP, DEEP, 0), (DEEP, middle_rows, 1)):
        for i, src in enumerate(inputs):
            pltpu.make_async_copy(
                src.at[pl.ds(first, count)], arrays.at[i, pl.ds(TOP + first, count), own], load_sem.at[group]
            ).start()

    barrier = pltpu.get_barrier_semaphore()
    expected = jnp.int32(0)
    for dy, dx in DIRECTIONS:
        there = exists(dy, dx)
        expected = expected + there.astype(jnp.int32)

        @pl.when(there)
        def _():
            pl.semaphore_signal(barrier, 1, device_id=(my + dy, mx + dx), device_id_type=MESH)

    for side, dy in enumerate((-1, 1)):
        @pl.when(~exists(dy, 0))
        def _():
            for number in range(ROUNDS):
                parcel_in[number, side] = jnp.zeros(parcel_in.shape[2:], jnp.float32)
        for other, dx in enumerate((-1, 1)):
            @pl.when(~exists(dy, dx))
            def _():
                for number in range(ROUNDS):
                    corner_in[number, side, other] = jnp.zeros(corner_in.shape[3:], jnp.float32)
    for dx in (-1, 1):
        @pl.when(~exists(0, dx))
        def _():
            start = pl.ds(0 if dx < 0 else PAD + columns, PAD)
            for i in range(4):
                arrays[i, pl.ds(TOP, rows), start] = jnp.zeros((rows, PAD, levels), jnp.float32)

    edges = (TOP, TOP + rows - 1)
    beyond = (TOP - 1, TOP + rows)

    def prepare(number, side):
        at = FIELD[number]
        edge, inward = edges[side], 1 - 2 * side
        second, third = edge + inward, edge + 2 * inward
        outer, middle = arrays[at, edge, own], arrays[at, second, own]
        place = lax.broadcasted_iota(jnp.int32, (columns, levels), 0)
        before = jnp.where(place == 0, 0.0, pltpu.roll(middle, 1, 0))
        after = jnp.where(place == columns - 1, 0.0, pltpu.roll(middle, columns - 1, 0))
        spread = (outer + arrays[at, third, own]) + (before + after) - 4.0 * middle
        second_rate = arrays[RATE, second, own]
        later = middle + second_rate * spread + arrays[GAIN, second, own]
        rate, gain = arrays[RATE, edge, own], arrays[GAIN, edge, own]
        term = rate * middle + gain
        out = parcel_out.at[number, side]
        out[pl.ds(0, columns)] = outer
        out[pl.ds(columns, columns)] = term
        out[pl.ds(2 * columns, columns)] = rate * later + gain
        if number == 0:
            out[pl.ds(3 * columns, columns)] = rate
            out[pl.ds(4 * columns, 1)] = second_rate[:1]
            out[pl.ds(4 * columns + 1, 1)] = second_rate[columns - 1:]
        for other in range(2):
            last = columns - 1 if other else 0
            beside = columns - 2 if other else 1
            cells = corner_out.at[number, side, other]
            cells[pl.ds(0, 1)] = outer[last:last + 1]
            cells[pl.ds(1, 1)] = outer[beside:beside + 1]
            cells[pl.ds(2, 1)] = middle[last:last + 1]
            cells[pl.ds(3, 1)] = term[last:last + 1]
            if number == 0:
                cells[pl.ds(4, 1)] = rate[last:last + 1]

    def remote(direction, src, dst, recv):
        return direction, pltpu.make_async_remote_copy(
            src_ref=src,
            dst_ref=dst,
            send_sem=send_sem.at[DIRECTIONS.index(direction)],
            recv_sem=recv,
            device_id=(my + direction[0], mx + direction[1]),
            device_id_type=MESH,
        )

    def to_side(number, side):
        dy, there = 2 * side - 1, 1 - side
        out = []
        for other, dx in enumerate((-1, 1)):
            cells = pl.ds(0, CORNER[number])
            out.append(remote((dy, dx), corner_out.at[number, side, other, cells],
                              corner_in.at[number, there, 1 - other, cells], side_sem.at[number, there, 2 - other]))
        size = pl.ds(0, parcel(number, columns))
        out.append(remote((dy, 0), parcel_out.at[number, side, size], parcel_in.at[number, there, size],
                          side_sem.at[number, there, 0]))
        return out

    def start(copies):
        for (dy, dx), copy in copies:
            @pl.when(exists(dy, dx))
            def _():
                copy.start()

    def wait_side(number, side):
        for (dy, dx), copy in to_side(number, 1 - side):
            @pl.when(exists(-dy, -dx))
            def _():
                copy.wait_recv()

    def sideways(number, first, count):
        out = []
        for other, dx in enumerate((-1, 1)):
            for i, reach in ((FIELD[number], 3),) + (((RATE, 2), (GAIN, 2)) if number == 0 else ()):
                from_ = PAD if dx < 0 else PAD + columns - reach
                to = PAD + columns if dx < 0 else PAD - reach
                out.append(remote((0, dx), arrays.at[i, pl.ds(first, count), pl.ds(from_, reach)],
                                  arrays.at[i, pl.ds(first, count), pl.ds(to, reach)], across_sem.at[number, 1 - other]))
        return out

    flat_all = arrays.reshape(4 * tall * width, levels)

    def settle(sem, count):
        some = flat_all.at[pl.ds(0, count)]
        pltpu.make_async_copy(some, some, sem).wait()

    def wait_across(number):
        for other, dx in enumerate((-1, 1)):
            @pl.when(exists(0, dx))
            def _():
                settle(across_sem.at[number, other], rows * (7 if number == 0 else 3))

    flat_rate = arrays.at[RATE].reshape(tall * width, levels)
    flat_gain = arrays.at[GAIN].reshape(tall * width, levels)

    def advance(old, first, count, column, wide, put, carry):
        flat = old.reshape(tall * width, levels)

        def row(i, state):
            above, middle, carry = state
            at = (first + i) * width + column
            below = flat[pl.ds(at + width, wide), :]
            sides = flat[pl.ds(at - 1, wide), :] + flat[pl.ds(at + 1, wide), :]
            spread = (above + below) + sides - 4.0 * middle
            later = middle + flat_rate[pl.ds(at, wide), :] * spread + flat_gain[pl.ds(at, wide), :]
            return middle, below, put(first - TOP + i, later, carry)

        at = first * width + column
        state = (flat[pl.ds(at - width, wide), :], flat[pl.ds(at, wide), :], carry)
        return lax.fori_loop(0, count, row, state, unroll=min(count, 4))[2]

    def advance_beyond(side, step, old, new):
        flat = old.reshape(tall * width, levels)
        at = beyond[side] * width
        inward = edges[side] * width
        middle = flat[pl.ds(at, width), :]
        sides = flat[pl.ds(at - 1, width), :] + flat[pl.ds(at + 1, width), :]
        spread = flat[pl.ds(inward, width), :] + sides - 4.0 * middle
        later = middle + flat_rate[pl.ds(at, width), :] * spread + extra[side, step]
        new.reshape(tall * width, levels)[pl.ds(at, width), :] = later

    def unpack(number, side):
        at, far = FIELD[number], beyond[side]
        came = parcel_in.at[number, side]
        arrays[at, far, own] = came[pl.ds(0, columns)]
        extra[side, 0, own] = came[pl.ds(columns, columns)]
        extra[side, 1, own] = came[pl.ds(2 * columns, columns)]
        if number == 0:
            arrays[RATE, far, own] = came[pl.ds(3 * columns, columns)]
        for other in range(2):
            cells = corner_in.at[number, side, other]
            last = pl.ds(PAD + columns - 1 if other else PAD, 1)
            near = pl.ds(PAD + columns if other else PAD - 1, 1)
            next_ = pl.ds(PAD + columns + 1 if other else PAD - 2, 1)
            arrays[at, far, near] = cells[pl.ds(0, 1)]
            arrays[at, far, next_] = cells[pl.ds(1, 1)]
            extra[side, 0, near] = cells[pl.ds(3, 1)]
            if number == 0:
                arrays[RATE, far, near] = cells[pl.ds(4, 1)]
            second_rate = parcel_in[0, side, pl.ds(4 * columns + other, 1)]
            extra[side, 1, last] = extra[side, 1, last] + (arrays[RATE, far, last] * second_rate) * cells[pl.ds(2, 1)]

    def announce(index):
        if index < len(reaches):
            for dy in (-reaches[index], reaches[index]):
                @pl.when(exists(dy, 0))
                def _():
                    pl.semaphore_signal(present.at[index], 1, device_id=(my + dy, mx), device_id_type=MESH)

    def hear(index):
        if index < len(reaches):
            count = exists(-reaches[index], 0).astype(jnp.int32) + exists(reaches[index], 0).astype(jnp.int32)
            pl.semaphore_wait(present.at[index], count)

    settle(load_sem.at[0], 3 * 2 * DEEP * columns)
    for side in range(2):
        prepare(0, side)
    pl.semaphore_wait(barrier, expected)
    for side in range(2):
        start(to_side(0, side))
    announce(0)
    settle(load_sem.at[1], 3 * middle_rows * columns)
    start(sideways(0, TOP, rows))

    total = jnp.zeros((columns, levels), jnp.float32)
    for number in range(ROUNDS):
        wait_across(number)
        hear(2 * number)
        announce(2 * number + 1)
        for part in ("inside", "low", "high"):
            side = None if part == "inside" else (0 if part == "low" else 1)
            if side is not None:
                wait_side(number, side)
                unpack(number, side)
            old = arrays.at[FIELD[number]]
            for step in range(DEEP):
                last = step == DEEP - 1
                if part == "inside":
                    first, count = TOP + step + 1, rows - 2 * (step + 1)
                elif part == "low":
                    first, count = TOP, step + 1
                else:
                    first, count = TOP + rows - step - 1, step + 1
                column, wide, new = 0, width, None
                if not last:
                    new = work.at[step]
                else:
                    column, wide = PAD, columns
                    if number < ROUNDS - 1:
                        new = arrays.at[FIELD[number + 1]]

                def put(i, later, carry, new=new, column=column, wide=wide):
                    if new is None:
                        density_out[i] = later
                        return carry + later
                    new.reshape(tall * width, levels)[pl.ds((TOP + i) * width + column, wide), :] = later
                    return carry

                total = advance(old, first, count, column, wide, put, total)
                if side is not None and not last:
                    advance_beyond(side, step, old, new)
                old = new
            if number < ROUNDS - 1:
                if side is None:
                    start(sideways(number + 1, TOP + DEEP, middle_rows))
                else:
                    prepare(number + 1, side)
                    start(to_side(number + 1, side))
                    start(sideways(number + 1, TOP if side == 0 else TOP + rows - DEEP, DEEP))
        if number < ROUNDS - 1:
            hear(1)
            announce(2)

    local_mean = total * (1.0 / rows)

    def square(i, carry):
        away = density_out[i] - local_mean
        return carry + away * away

    squares = lax.fori_loop(0, rows, square, jnp.zeros((columns, levels), jnp.float32), unroll=4)
    stats[0, 0] = local_mean
    stats[0, 1] = squares
    for index in range(3, len(reaches)):
        hear(index)
        announce(index + 1)
    outer = py // inner
    far_first = sorted(
        ((do, di) for do in range(outer) for di in range(inner) if do or di),
        key=lambda place: -(min(place[0], outer - place[0]) + min(place[1], inner - place[1])),
    )
    for do, di in far_first:
        step = do * inner + di
        peer = lax.rem(my // inner + do, outer) * inner + lax.rem(lax.rem(my, inner) + di, inner)
        pltpu.make_async_remote_copy(
            src_ref=stats.at[0],
            dst_ref=stats.at[step],
            send_sem=stat_sem.at[0],
            recv_sem=stat_sem.at[1],
            device_id=(peer, mx),
            device_id_type=MESH,
        ).start()
    for d, (dy, dx) in enumerate(DIRECTIONS):
        @pl.when(exists(dy, dx))
        def _():
            if dy and dx:
                count = sum(CORNER)
            elif dy:
                count = parcel(0, columns) + parcel(1, columns)
            else:
                count = 10 * rows
            settle(send_sem.at[d], count)
    others = stats.at[pl.ds(1, py - 1)]
    pltpu.make_async_copy(others, others, stat_sem.at[1]).wait()
    mean = stats[0, 0]
    for step in range(1, py):
        mean = mean + stats[step, 0]
    mean = mean * (1.0 / py)
    inside = stats[0, 1]
    between = (stats[0, 0] - mean) * (stats[0, 0] - mean)
    for step in range(1, py):
        inside = inside + stats[step, 1]
        between = between + (stats[step, 0] - mean) * (stats[step, 0] - mean)
    variance = inside * (1.0 / (rows * py)) + between * (1.0 / py)
    mean_out[...] = mean
    scale_out[...] = lax.rsqrt(variance + 0.0001)
    pltpu.make_async_copy(others, others, stat_sem.at[0]).wait()

CHUNKS = 2


def finish(density, mean, scale, anomaly_out, density_out, anomaly, sem):
    rows = density.shape[0]
    whole = pltpu.make_async_copy(density, density_out, sem.at[CHUNKS])
    whole.start()
    part = rows // CHUNKS
    copies = []
    for chunk in range(CHUNKS):
        for i in range(chunk * part, (chunk + 1) * part):
            anomaly[i] = (density[i] - mean[...]) * scale[...]
        own = pl.ds(chunk * part, part)
        copies.append(pltpu.make_async_copy(anomaly.at[own], anomaly_out.at[own], sem.at[chunk]))
        copies[-1].start()
    for copy in copies:
        copy.wait()
    whole.wait()


def per_device(py, px, inner, density, conductance, source):
    rows, columns, levels = density.shape
    tall, width = rows + 2 * TOP, columns + 2 * PAD
    vmem = pl.BlockSpec(memory_space=pltpu.VMEM)
    line = jax.ShapeDtypeStruct((columns, levels), jnp.float32)
    density, conductance, source = (pltpu.with_memory_space_constraint(x, pltpu.HBM) for x in (density, conductance, source))
    density, mean, scale = pl.pallas_call(
        functools.partial(kernel, py, px, inner),
        out_shape=[jax.ShapeDtypeStruct(density.shape, jnp.float32), line, line],
        in_specs=[pl.BlockSpec(memory_space=pltpu.HBM)] * 3,
        out_specs=[vmem] * 3,
        scratch_shapes=[
            pltpu.VMEM((4, tall, width, levels), jnp.float32),
            pltpu.VMEM((DEEP - 1, tall, width, levels), jnp.float32),
            pltpu.VMEM((2, 2, width, levels), jnp.float32),
            pltpu.VMEM((ROUNDS, 2, 4 * columns + 8, levels), jnp.float32),
            pltpu.VMEM((ROUNDS, 2, 4 * columns + 8, levels), jnp.float32),
            pltpu.VMEM((ROUNDS, 2, 2, 8, levels), jnp.float32),
            pltpu.VMEM((ROUNDS, 2, 2, 8, levels), jnp.float32),
            pltpu.VMEM((py, 2, columns, levels), jnp.float32),
            pltpu.SemaphoreType.DMA((2,)),
            pltpu.SemaphoreType.DMA((len(DIRECTIONS),)),
            pltpu.SemaphoreType.DMA((ROUNDS, 2, 3)),
            pltpu.SemaphoreType.DMA((ROUNDS, 2)),
            pltpu.SemaphoreType.DMA((2,)),
            pltpu.SemaphoreType.REGULAR((max(1, len(reaches_of(py))),)),
        ],
        compiler_params=pltpu.CompilerParams(collective_id=0, has_side_effects=True, vmem_limit_bytes=10*2**20),
    )(density, conductance, source)
    return pl.pallas_call(
        finish,
        out_shape=[jax.ShapeDtypeStruct(density.shape, jnp.float32)] * 2,
        in_specs=[vmem] * 3,
        out_specs=[pl.BlockSpec(memory_space=pltpu.HBM)] * 2,
        scratch_shapes=[pltpu.VMEM(density.shape, jnp.float32), pltpu.SemaphoreType.DMA((CHUNKS + 1,))],
        compiler_params=pltpu.CompilerParams(vmem_limit_bytes=4 * 2**20),
    )(density, mean, scale)


def solution(mesh):
    spec = P("py", "px", None)
    line = mesh.devices.reshape(mesh.shape["py"], -1)[:, 0] if mesh.axis_names[0] == "py" else []
    places = [getattr(device, "coords", (0, 0, 0))[2] for device in line]
    inner = max(1, places.count(places[0])) if places else 1
    return jax.shard_map(
        functools.partial(per_device, mesh.shape["py"], mesh.shape["px"], inner),
        mesh=mesh, in_specs=(spec,) * 3, out_specs=(spec,) * 2, check_vma=False,
    )
```

```python
import functools

import jax
import jax.numpy as jnp
from jax import lax
from jax.experimental import pallas as pl
from jax.experimental.pallas import tpu as pltpu
from jax.sharding import PartitionSpec as P

ROUNDS = 2
DEEP = 3
PAD = 4
TOP = 2
DIRECTIONS = [(-1, 0), (1, 0), (-1, -1), (-1, 1), (1, -1), (1, 1), (0, -1), (0, 1)]
MESH = pl.DeviceIdType.MESH
FIELD = (0, 3)
RATE, GAIN = 1, 2
CORNER = (5, 4)
ZONE = 2 * DEEP


def reaches_of(py):
    known, reaches = 1, []
    while known < py - 1:
        reaches.append(known)
        known *= 2
    return reaches


def parcel(number, half, columns):
    return (4 if number == 0 else 3) * (columns // 2) + (2 if number == 0 and half == 0 else 0)


def kernel(py, px, inner, field, conductance, source, density_out, mean_out, scale_out,
           arrays, work, extra, parcel_out, parcel_in, corner_out, corner_in, stats,
           load_sem, send_sem, side_sem, across_sem, stat_sem, present):
    rows, columns, levels = field.shape
    width = columns + 2 * PAD
    tall = rows + 2 * TOP
    my, mx = lax.axis_index("py"), lax.axis_index("px")
    reaches = reaches_of(py)

    def exists(dy, dx):
        here = jnp.bool_(True)
        if dy:
            here = here & ((my + dy >= 0) if dy < 0 else (my + dy < py))
        if dx:
            here = here & ((mx + dx >= 0) if dx < 0 else (mx + dx < px))
        return here

    barrier = pltpu.get_barrier_semaphore()
    expected = jnp.int32(0)
    for dy, dx in DIRECTIONS:
        there = exists(dy, dx)
        expected = expected + there.astype(jnp.int32)

        @pl.when(there)
        def _():
            pl.semaphore_signal(barrier, 1, device_id=(my + dy, mx + dx), device_id_type=MESH)

    own = pl.ds(PAD, columns)
    middle_rows = rows - 2 * DEEP
    inputs = (field, conductance, source)
    for first, count, group in ((0, DEEP, 0), (rows - DEEP, DEEP, 0), (DEEP, middle_rows, 1)):
        for i, src in enumerate(inputs):
            pltpu.make_async_copy(
                src.at[pl.ds(first, count)], arrays.at[i, pl.ds(TOP + first, count), own], load_sem.at[group]
            ).start()

    for side, dy in enumerate((-1, 1)):
        @pl.when(~exists(dy, 0))
        def _():
            parcel_in[:, side] = jnp.zeros(parcel_in.shape[:1] + parcel_in.shape[2:], jnp.float32)
        for other, dx in enumerate((-1, 1)):
            @pl.when(~exists(dy, dx))
            def _():
                for turn in range(3):
                    corner_in[turn, side, other] = jnp.zeros(corner_in.shape[3:], jnp.float32)
    for dx in (-1, 1):
        @pl.when(~exists(0, dx))
        def _():
            start = pl.ds(0 if dx < 0 else PAD + columns, PAD)
            for i in range(4):
                arrays[i, pl.ds(TOP, rows), start] = jnp.zeros((rows, PAD, levels), jnp.float32)

    edges = (TOP, TOP + rows - 1)
    beyond = (TOP - 1, TOP + rows)

    half_columns, half_levels = columns // 2, levels // 2
    low_half = lax.broadcasted_iota(jnp.int32, (half_columns, levels), 1) < half_levels

    def fold(value, half):
        first, second = value[:half_columns], value[half_columns:]
        if half == 0:
            return jnp.where(low_half, first, pltpu.roll(second, half_levels, 1))
        return jnp.where(low_half, pltpu.roll(first, half_levels, 1), second)

    def unfold(first, second=None):
        turned = pltpu.roll(first, half_levels, 1)
        if second is None:
            return first, turned
        back = pltpu.roll(second, half_levels, 1)
        return jnp.where(low_half, first, back), jnp.where(low_half, turned, second)

    def prepare(number, side, halves):
        at = FIELD[number]
        edge, inward = edges[side], 1 - 2 * side
        second, third = edge + inward, edge + 2 * inward
        outer, middle = arrays[at, edge, own], arrays[at, second, own]
        place = lax.broadcasted_iota(jnp.int32, (columns, levels), 0)
        before = jnp.where(place == 0, 0.0, pltpu.roll(middle, 1, 0))
        after = jnp.where(place == columns - 1, 0.0, pltpu.roll(middle, columns - 1, 0))
        spread = (outer + arrays[at, third, own]) + (before + after) - 4.0 * middle
        second_rate = arrays[RATE, second, own]
        later = middle + second_rate * spread + arrays[GAIN, second, own]
        rate, gain = arrays[RATE, edge, own], arrays[GAIN, edge, own]
        term = rate * middle + gain
        values = [outer, term, rate * later + gain] + ([rate] if number == 0 else [])
        for half in halves:
            out = parcel_out.at[2 * number + half, side]
            for i, value in enumerate(values):
                out[pl.ds(i * half_columns, half_columns)] = fold(value, half)
            if number == 0 and half == 0:
                out[pl.ds(4 * half_columns, 1)] = second_rate[:1]
                out[pl.ds(4 * half_columns + 1, 1)] = second_rate[columns - 1:]
        for other in range(2):
            last = columns - 1 if other else 0
            beside = columns - 2 if other else 1
            cells = corner_out.at[number + halves[0], side, other]
            cells[pl.ds(0, 1)] = outer[last:last + 1]
            cells[pl.ds(1, 1)] = outer[beside:beside + 1]
            cells[pl.ds(2, 1)] = middle[last:last + 1]
            cells[pl.ds(3, 1)] = term[last:last + 1]
            if number == 0:
                cells[pl.ds(4, 1)] = rate[last:last + 1]

    def remote(direction, src, dst, recv):
        return direction, pltpu.make_async_remote_copy(
            src_ref=src,
            dst_ref=dst,
            send_sem=send_sem.at[DIRECTIONS.index(direction)],
            recv_sem=recv,
            device_id=(my + direction[0], mx + direction[1]),
            device_id_type=MESH,
        )

    def corners(number, half, side):
        dy, there, turn = 2 * side - 1, 1 - side, number * (half + 1)
        cells = pl.ds(0, CORNER[number])
        return [remote((dy, dx), corner_out.at[turn, side, other, cells], corner_in.at[turn, there, 1 - other, cells],
                       side_sem.at[there, 4 + 2 * turn + 1 - other]) for other, dx in enumerate((-1, 1))]

    def rows_of(number, half, side):
        dy, there, size = 2 * side - 1, 1 - side, pl.ds(0, parcel(number, half, columns))
        slot = 2 * number + half
        return [remote((dy, 0), parcel_out.at[slot, side, size], parcel_in.at[slot, there, size], side_sem.at[there, slot])]

    def start(copies):
        for (dy, dx), copy in copies:
            @pl.when(exists(dy, dx))
            def _():
                copy.start()

    def wait_side(number, half, side):
        copies = rows_of(number, half, 1 - side)
        if number or not half:
            copies = copies + corners(number, half, 1 - side)
        for (dy, dx), copy in copies:
            @pl.when(exists(-dy, -dx))
            def _():
                copy.wait_recv()

    def sideways(number, group, first, count):
        out = []
        for other, dx in enumerate((-1, 1)):
            for i, reach in ((FIELD[number], 3),) + (((RATE, 2), (GAIN, 2)) if number == 0 else ()):
                from_ = PAD if dx < 0 else PAD + columns - reach
                to = PAD + columns if dx < 0 else PAD - reach
                out.append(remote((0, dx), arrays.at[i, pl.ds(first, count), pl.ds(from_, reach)],
                                  arrays.at[i, pl.ds(first, count), pl.ds(to, reach)], across_sem.at[group, 1 - other]))
        return out

    flat_all = arrays.reshape(4 * tall * width, levels)

    def settle(sem, count):
        some = flat_all.at[pl.ds(0, count)]
        pltpu.make_async_copy(some, some, sem).wait()

    def wait_across(group, count):
        for other, dx in enumerate((-1, 1)):
            @pl.when(exists(0, dx))
            def _():
                settle(across_sem.at[group, other], count)

    flat_rate = arrays.at[RATE].reshape(tall * width, levels)
    flat_gain = arrays.at[GAIN].reshape(tall * width, levels)

    def advance(old, first, count, column, wide, put, carry):
        flat = old.reshape(tall * width, levels)

        def row(i, state):
            above, middle, carry = state
            at = (first + i) * width + column
            below = flat[pl.ds(at + width, wide), :]
            sides = flat[pl.ds(at - 1, wide), :] + flat[pl.ds(at + 1, wide), :]
            spread = (above + below) + sides - 4.0 * middle
            later = middle + flat_rate[pl.ds(at, wide), :] * spread + flat_gain[pl.ds(at, wide), :]
            return middle, below, put(first - TOP + i, later, carry)

        at = first * width + column
        state = (flat[pl.ds(at - width, wide), :], flat[pl.ds(at, wide), :], carry)
        return lax.fori_loop(0, count, row, state, unroll=min(count, 4))[2]

    def advance_beyond(side, step, old, new):
        flat = old.reshape(tall * width, levels)
        at = beyond[side] * width
        inward = edges[side] * width
        middle = flat[pl.ds(at, width), :]
        sides = flat[pl.ds(at - 1, width), :] + flat[pl.ds(at + 1, width), :]
        spread = flat[pl.ds(inward, width), :] + sides - 4.0 * middle
        later = middle + flat_rate[pl.ds(at, width), :] * spread + extra[side, step]
        new.reshape(tall * width, levels)[pl.ds(at, width), :] = later

    def unpack(number, half, side):
        at, far = FIELD[number], beyond[side]
        came = [parcel_in.at[2 * number + i, side] for i in range(half + 1)]
        targets = [arrays.at[at, far], extra.at[side, 0], extra.at[side, 1]] + ([arrays.at[RATE, far]] if number == 0 else [])
        for i, target in enumerate(targets):
            parts = unfold(*[one[pl.ds(i * half_columns, half_columns)] for one in came])
            for part in range(2):
                target[pl.ds(PAD + part * half_columns, half_columns)] = parts[part]
        for other in range(2):
            cells = corner_in.at[number * (half + 1), side, other]
            last = pl.ds(PAD + columns - 1 if other else PAD, 1)
            near = pl.ds(PAD + columns if other else PAD - 1, 1)
            next_ = pl.ds(PAD + columns + 1 if other else PAD - 2, 1)
            arrays[at, far, near] = cells[pl.ds(0, 1)]
            arrays[at, far, next_] = cells[pl.ds(1, 1)]
            extra[side, 0, near] = cells[pl.ds(3, 1)]
            if number == 0:
                arrays[RATE, far, near] = cells[pl.ds(4, 1)]
            second_rate = parcel_in[0, side, pl.ds(4 * half_columns + other, 1)]
            extra[side, 1, last] = extra[side, 1, last] + (arrays[RATE, far, last] * second_rate) * cells[pl.ds(2, 1)]

    def announce(index):
        if index < len(reaches):
            for dy in (-reaches[index], reaches[index]):
                @pl.when(exists(dy, 0))
                def _():
                    pl.semaphore_signal(present.at[index], 1, device_id=(my + dy, mx), device_id_type=MESH)

    def hear(index):
        if index < len(reaches):
            count = exists(-reaches[index], 0).astype(jnp.int32) + exists(reaches[index], 0).astype(jnp.int32)
            pl.semaphore_wait(present.at[index], count)

    def steps(number, bands, side, carry):
        old = arrays.at[FIELD[number]]
        for step, (first, count) in enumerate(bands):
            last = step == DEEP - 1
            column, wide, new = 0, width, None
            if not last:
                new = work.at[step]
            else:
                column, wide = PAD, columns
                if number < ROUNDS - 1:
                    new = arrays.at[FIELD[number + 1]]

            def put(i, later, carry, new=new, column=column, wide=wide):
                if new is None:
                    density_out[i] = later
                    if carry is None:
                        return None
                    pivot, once, twice = carry
                    away = later - pivot
                    return pivot, once + away, twice + away * away
                new.reshape(tall * width, levels)[pl.ds((TOP + i) * width + column, wide), :] = later
                return carry

            if new is None and carry is None:
                advance(old, first, 1, column, wide, put, None)
                zero = jnp.zeros((columns, levels), jnp.float32)
                carry = density_out[first - TOP], zero, zero
                first, count = first + 1, count - 1
            carry = advance(old, first, count, column, wide, put, carry)
            if side is not None and not last:
                advance_beyond(side, step, old, new)
            old = new
        return carry

    def bands(part, start, growth):
        out = []
        for step in range(DEEP):
            depth = start + growth * step
            if part == "inside":
                out.append((TOP + depth, rows - 2 * depth))
            else:
                out.append((TOP if part == 0 else TOP + rows - depth, depth))
        return out

    settle(load_sem.at[0], 3 * 2 * DEEP * columns)
    for side in range(2):
        prepare(0, side, (0, 1))
    pl.semaphore_wait(barrier, expected)
    for side in range(2):
        start(corners(0, 0, side))
    for half in range(2):
        for side in range(2):
            start(rows_of(0, half, side))
    announce(0)
    settle(load_sem.at[1], 3 * middle_rows * columns)
    for side in range(2):
        start(sideways(0, 0, TOP + side * (rows - ZONE), ZONE))
    start(sideways(0, 1, TOP + ZONE, rows - 2 * ZONE))
    hear(0)
    announce(1)
    wait_across(0, 2 * ZONE * 7)
    for half in range(2):
        for side in range(2):
            wait_side(0, half, side)
            unpack(0, half, side)
            steps(0, bands(side, ZONE - 1, -1), side, ())
            prepare(1, side, (half,))
            start(corners(1, half, side) + rows_of(1, half, side))
            if half:
                start(sideways(1, 2, TOP + side * (rows - DEEP), DEEP))
        if half == 0:
            hear(1)
            announce(2)
    wait_across(1, (rows - 2 * ZONE) * 7)
    steps(0, bands("inside", ZONE - 1, -1), None, ())
    start(sideways(1, 2, TOP + DEEP, middle_rows))
    wait_across(2, rows * 3)
    within = steps(1, bands("inside", 1, 1), None, None)
    for index in range(2, len(reaches)):
        hear(index)
        announce(index + 1)
    outer = py // inner
    far_first = sorted(
        ((do, di) for do in range(outer) for di in range(inner) if do or di),
        key=lambda place: -(min(place[0], outer - place[0]) + min(place[1], inner - place[1])),
    )
    for half in range(2):
        sums = within
        for side in range(2):
            wait_side(1, half, side)
            unpack(1, half, side)
            sums = steps(1, bands(side, 1, 1), side, sums)
        pivot, once, twice = sums
        shift = once * (1.0 / rows)
        stats[half, 0, pl.ds(0, half_columns)] = fold(pivot + shift, half)
        stats[half, 0, pl.ds(half_columns, half_columns)] = fold(twice - once * shift, half)
        for do, di in far_first:
            step = do * inner + di
            peer = lax.rem(my // inner + do, outer) * inner + lax.rem(lax.rem(my, inner) + di, inner)
            pltpu.make_async_remote_copy(
                src_ref=stats.at[half, 0],
                dst_ref=stats.at[half, step],
                send_sem=stat_sem.at[2],
                recv_sem=stat_sem.at[half],
                device_id=(peer, mx),
                device_id_type=MESH,
            ).start()
    for d, (dy, dx) in enumerate(DIRECTIONS):
        @pl.when(exists(dy, dx))
        def _():
            if dy and dx:
                count = CORNER[0] + 2 * CORNER[1]
            elif dy:
                count = sum(parcel(number, half, columns) for number in range(ROUNDS) for half in range(2))
            else:
                count = 10 * rows
            settle(send_sem.at[d], count)
    means, scales = [], []
    for half in range(2):
        settle(stat_sem.at[half], (py - 1) * columns)
        came = [(stats[half, step, pl.ds(0, half_columns)], stats[half, step, pl.ds(half_columns, half_columns)])
                for step in range(py)]
        mean = came[0][0]
        for one, _ in came[1:]:
            mean = mean + one
        mean = mean * (1.0 / py)
        inside = came[0][1]
        between = (came[0][0] - mean) * (came[0][0] - mean)
        for one, squares in came[1:]:
            inside = inside + squares
            between = between + (one - mean) * (one - mean)
        variance = inside * (1.0 / (rows * py)) + between * (1.0 / py)
        means.append(mean)
        scales.append(lax.rsqrt(variance + 0.0001))
    for out, parts in ((mean_out, unfold(*means)), (scale_out, unfold(*scales))):
        for part in range(2):
            out[pl.ds(part * half_columns, half_columns)] = parts[part]
    settle(stat_sem.at[2], 2 * (py - 1) * columns)

CHUNKS = 2


def finish(density, mean, scale, anomaly_out, density_out, anomaly, sem):
    rows = density.shape[0]
    whole = pltpu.make_async_copy(density, density_out, sem.at[CHUNKS])
    whole.start()
    part = rows // CHUNKS
    copies = []
    for chunk in range(CHUNKS):
        for i in range(chunk * part, (chunk + 1) * part):
            anomaly[i] = (density[i] - mean[...]) * scale[...]
        own = pl.ds(chunk * part, part)
        copies.append(pltpu.make_async_copy(anomaly.at[own], anomaly_out.at[own], sem.at[chunk]))
        copies[-1].start()
    for copy in copies:
        copy.wait()
    whole.wait()


def per_device(py, px, inner, density, conductance, source):
    rows, columns, levels = density.shape
    tall, width = rows + 2 * TOP, columns + 2 * PAD
    vmem = pl.BlockSpec(memory_space=pltpu.VMEM)
    line = jax.ShapeDtypeStruct((columns, levels), jnp.float32)
    density, conductance, source = (pltpu.with_memory_space_constraint(x, pltpu.HBM) for x in (density, conductance, source))
    density, mean, scale = pl.pallas_call(
        functools.partial(kernel, py, px, inner),
        out_shape=[jax.ShapeDtypeStruct(density.shape, jnp.float32), line, line],
        in_specs=[pl.BlockSpec(memory_space=pltpu.HBM)] * 3,
        out_specs=[vmem] * 3,
        scratch_shapes=[
            pltpu.VMEM((4, tall, width, levels), jnp.float32),
            pltpu.VMEM((DEEP - 1, tall, width, levels), jnp.float32),
            pltpu.VMEM((2, 2, width, levels), jnp.float32),
            pltpu.VMEM((2 * ROUNDS, 2, 2 * columns + 8, levels), jnp.float32),
            pltpu.VMEM((2 * ROUNDS, 2, 2 * columns + 8, levels), jnp.float32),
            pltpu.VMEM((3, 2, 2, 8, levels), jnp.float32),
            pltpu.VMEM((3, 2, 2, 8, levels), jnp.float32),
            pltpu.VMEM((2, py, columns, levels), jnp.float32),
            pltpu.SemaphoreType.DMA((2,)),
            pltpu.SemaphoreType.DMA((len(DIRECTIONS),)),
            pltpu.SemaphoreType.DMA((2, 10)),
            pltpu.SemaphoreType.DMA((3, 2)),
            pltpu.SemaphoreType.DMA((3,)),
            pltpu.SemaphoreType.REGULAR((max(1, len(reaches_of(py))),)),
        ],
        compiler_params=pltpu.CompilerParams(collective_id=0, has_side_effects=True, vmem_limit_bytes=10*2**20),
    )(density, conductance, source)
    return pl.pallas_call(
        finish,
        out_shape=[jax.ShapeDtypeStruct(density.shape, jnp.float32)] * 2,
        in_specs=[vmem] * 3,
        out_specs=[pl.BlockSpec(memory_space=pltpu.HBM)] * 2,
        scratch_shapes=[pltpu.VMEM(density.shape, jnp.float32), pltpu.SemaphoreType.DMA((CHUNKS + 1,))],
        compiler_params=pltpu.CompilerParams(vmem_limit_bytes=4 * 2**20),
    )(density, mean, scale)


def solution(mesh):
    spec = P("py", "px", None)
    line = mesh.devices.reshape(mesh.shape["py"], -1)[:, 0] if mesh.axis_names[0] == "py" else []
    places = [getattr(device, "coords", (0, 0, 0))[2] for device in line]
    inner = max(1, places.count(places[0])) if places else 1
    return jax.shard_map(
        functools.partial(per_device, mesh.shape["py"], mesh.shape["px"], inner),
        mesh=mesh, in_specs=(spec,) * 3, out_specs=(spec,) * 2, check_vma=False,
    )
```

```python
import functools

import jax
import jax.numpy as jnp
from jax import lax
from jax.experimental import pallas as pl
from jax.experimental.pallas import tpu as pltpu
from jax.sharding import PartitionSpec as P

ROUNDS = 2
DEEP = 3
PAD = 4
TOP = 2
DIRECTIONS = [(-1, 0), (1, 0), (-1, -1), (-1, 1), (1, -1), (1, 1), (0, -1), (0, 1)]
MESH = pl.DeviceIdType.MESH
FIELD = (0, 3)
RATE, GAIN = 1, 2
CORNER = (5, 4)


def reaches_of(py):
    known, reaches = 1, []
    while known < py - 1:
        reaches.append(known)
        known *= 2
    return reaches


def order_of(py, inner):
    if (py, inner) == (8, 2):
        return [5, 4, 3, 2, 6, 1, 7]
    outer = py // inner
    places = [(do, di) for do in range(outer) for di in range(inner) if do or di]
    places.sort(key=lambda place: -(min(place[0], outer - place[0]) + min(place[1], inner - place[1])))
    return [do * inner + di for do, di in places]


def parcel(number, columns):
    return (4 if number == 0 else 3) * columns + (2 if number == 0 else 0)


def kernel(py, px, inner, field, conductance, source, density_out, mean_out, scale_out,
           arrays, work, extra, parcel_out, parcel_in, corner_out, corner_in, stats,
           load_sem, send_sem, side_sem, across_sem, stat_sem, present):
    rows, columns, levels = field.shape
    width = columns + 2 * PAD
    tall = rows + 2 * TOP
    my, mx = lax.axis_index("py"), lax.axis_index("px")
    reaches = reaches_of(py)

    def exists(dy, dx):
        here = jnp.bool_(True)
        if dy:
            here = here & ((my + dy >= 0) if dy < 0 else (my + dy < py))
        if dx:
            here = here & ((mx + dx >= 0) if dx < 0 else (mx + dx < px))
        return here

    barrier = pltpu.get_barrier_semaphore()
    expected = jnp.int32(0)
    for dy, dx in DIRECTIONS:
        there = exists(dy, dx)
        expected = expected + there.astype(jnp.int32)

        @pl.when(there)
        def _():
            pl.semaphore_signal(barrier, 1, device_id=(my + dy, mx + dx), device_id_type=MESH)

    own = pl.ds(PAD, columns)
    middle_rows = rows - 2 * DEEP
    inputs = (field, conductance, source)
    for first, count, group in ((0, DEEP, 0), (rows - DEEP, DEEP, 0), (DEEP, middle_rows, 1)):
        for i, src in enumerate(inputs):
            pltpu.make_async_copy(
                src.at[pl.ds(first, count)], arrays.at[i, pl.ds(TOP + first, count), own], load_sem.at[group]
            ).start()

    for side, dy in enumerate((-1, 1)):
        @pl.when(~exists(dy, 0))
        def _():
            for number in range(ROUNDS):
                parcel_in[number, side] = jnp.zeros(parcel_in.shape[2:], jnp.float32)
        for other, dx in enumerate((-1, 1)):
            @pl.when(~exists(dy, dx))
            def _():
                for number in range(ROUNDS):
                    corner_in[number, side, other] = jnp.zeros(corner_in.shape[3:], jnp.float32)
    for dx in (-1, 1):
        @pl.when(~exists(0, dx))
        def _():
            start = pl.ds(0 if dx < 0 else PAD + columns, PAD)
            for i in range(4):
                arrays[i, pl.ds(TOP, rows), start] = jnp.zeros((rows, PAD, levels), jnp.float32)

    edges = (TOP, TOP + rows - 1)
    beyond = (TOP - 1, TOP + rows)

    def prepare(number, side):
        at = FIELD[number]
        edge, inward = edges[side], 1 - 2 * side
        second, third = edge + inward, edge + 2 * inward
        outer, middle = arrays[at, edge, own], arrays[at, second, own]
        place = lax.broadcasted_iota(jnp.int32, (columns, levels), 0)
        before = jnp.where(place == 0, 0.0, pltpu.roll(middle, 1, 0))
        after = jnp.where(place == columns - 1, 0.0, pltpu.roll(middle, columns - 1, 0))
        spread = (outer + arrays[at, third, own]) + (before + after) - 4.0 * middle
        second_rate = arrays[RATE, second, own]
        later = middle + second_rate * spread + arrays[GAIN, second, own]
        rate, gain = arrays[RATE, edge, own], arrays[GAIN, edge, own]
        term = rate * middle + gain
        out = parcel_out.at[number, side]
        out[pl.ds(0, columns)] = outer
        out[pl.ds(columns, columns)] = term
        out[pl.ds(2 * columns, columns)] = rate * later + gain
        if number == 0:
            out[pl.ds(3 * columns, columns)] = rate
            out[pl.ds(4 * columns, 1)] = second_rate[:1]
            out[pl.ds(4 * columns + 1, 1)] = second_rate[columns - 1:]
        for other in range(2):
            last = columns - 1 if other else 0
            beside = columns - 2 if other else 1
            cells = corner_out.at[number, side, other]
            cells[pl.ds(0, 1)] = outer[last:last + 1]
            cells[pl.ds(1, 1)] = outer[beside:beside + 1]
            cells[pl.ds(2, 1)] = middle[last:last + 1]
            cells[pl.ds(3, 1)] = term[last:last + 1]
            if number == 0:
                cells[pl.ds(4, 1)] = rate[last:last + 1]

    def remote(direction, src, dst, recv):
        return direction, pltpu.make_async_remote_copy(
            src_ref=src,
            dst_ref=dst,
            send_sem=send_sem.at[DIRECTIONS.index(direction)],
            recv_sem=recv,
            device_id=(my + direction[0], mx + direction[1]),
            device_id_type=MESH,
        )

    def to_side(number, side):
        dy, there = 2 * side - 1, 1 - side
        out = []
        for other, dx in enumerate((-1, 1)):
            cells = pl.ds(0, CORNER[number])
            out.append(remote((dy, dx), corner_out.at[number, side, other, cells],
                              corner_in.at[number, there, 1 - other, cells], side_sem.at[number, there, 2 - other]))
        size = pl.ds(0, parcel(number, columns))
        out.append(remote((dy, 0), parcel_out.at[number, side, size], parcel_in.at[number, there, size],
                          side_sem.at[number, there, 0]))
        return out

    def start(copies):
        for (dy, dx), copy in copies:
            @pl.when(exists(dy, dx))
            def _():
                copy.start()

    def wait_side(number, side):
        for (dy, dx), copy in to_side(number, 1 - side):
            @pl.when(exists(-dy, -dx))
            def _():
                copy.wait_recv()

    def sideways(number, first, count):
        out = []
        for other, dx in enumerate((-1, 1)):
            for i, reach in ((FIELD[number], 3),) + (((RATE, 2), (GAIN, 2)) if number == 0 else ()):
                from_ = PAD if dx < 0 else PAD + columns - reach
                to = PAD + columns if dx < 0 else PAD - reach
                out.append(remote((0, dx), arrays.at[i, pl.ds(first, count), pl.ds(from_, reach)],
                                  arrays.at[i, pl.ds(first, count), pl.ds(to, reach)], across_sem.at[number, 1 - other]))
        return out

    flat_all = arrays.reshape(4 * tall * width, levels)

    def settle(sem, count):
        some = flat_all.at[pl.ds(0, count)]
        pltpu.make_async_copy(some, some, sem).wait()

    def wait_across(number):
        for other, dx in enumerate((-1, 1)):
            @pl.when(exists(0, dx))
            def _():
                settle(across_sem.at[number, other], rows * (7 if number == 0 else 3))

    flat_rate = arrays.at[RATE].reshape(tall * width, levels)
    flat_gain = arrays.at[GAIN].reshape(tall * width, levels)

    def advance(old, first, count, column, wide, put, carry):
        flat = old.reshape(tall * width, levels)

        def row(i, state):
            above, middle, carry = state
            at = (first + i) * width + column
            below = flat[pl.ds(at + width, wide), :]
            sides = flat[pl.ds(at - 1, wide), :] + flat[pl.ds(at + 1, wide), :]
            spread = (above + below) + sides - 4.0 * middle
            later = middle + flat_rate[pl.ds(at, wide), :] * spread + flat_gain[pl.ds(at, wide), :]
            return middle, below, put(first - TOP + i, later, carry)

        at = first * width + column
        state = (flat[pl.ds(at - width, wide), :], flat[pl.ds(at, wide), :], carry)
        return lax.fori_loop(0, count, row, state, unroll=min(count, 4))[2]

    def advance_beyond(side, step, old, new):
        flat = old.reshape(tall * width, levels)
        at = beyond[side] * width
        inward = edges[side] * width
        middle = flat[pl.ds(at, width), :]
        sides = flat[pl.ds(at - 1, width), :] + flat[pl.ds(at + 1, width), :]
        spread = flat[pl.ds(inward, width), :] + sides - 4.0 * middle
        later = middle + flat_rate[pl.ds(at, width), :] * spread + extra[side, step]
        new.reshape(tall * width, levels)[pl.ds(at, width), :] = later

    def unpack(number, side):
        at, far = FIELD[number], beyond[side]
        came = parcel_in.at[number, side]
        arrays[at, far, own] = came[pl.ds(0, columns)]
        extra[side, 0, own] = came[pl.ds(columns, columns)]
        extra[side, 1, own] = came[pl.ds(2 * columns, columns)]
        if number == 0:
            arrays[RATE, far, own] = came[pl.ds(3 * columns, columns)]
        for other in range(2):
            cells = corner_in.at[number, side, other]
            last = pl.ds(PAD + columns - 1 if other else PAD, 1)
            near = pl.ds(PAD + columns if other else PAD - 1, 1)
            next_ = pl.ds(PAD + columns + 1 if other else PAD - 2, 1)
            arrays[at, far, near] = cells[pl.ds(0, 1)]
            arrays[at, far, next_] = cells[pl.ds(1, 1)]
            extra[side, 0, near] = cells[pl.ds(3, 1)]
            if number == 0:
                arrays[RATE, far, near] = cells[pl.ds(4, 1)]
            second_rate = parcel_in[0, side, pl.ds(4 * columns + other, 1)]
            extra[side, 1, last] = extra[side, 1, last] + (arrays[RATE, far, last] * second_rate) * cells[pl.ds(2, 1)]

    def announce(index):
        if index < len(reaches):
            for dy in (-reaches[index], reaches[index]):
                @pl.when(exists(dy, 0))
                def _():
                    pl.semaphore_signal(present.at[index], 1, device_id=(my + dy, mx), device_id_type=MESH)

    def hear(index):
        if index < len(reaches):
            count = exists(-reaches[index], 0).astype(jnp.int32) + exists(reaches[index], 0).astype(jnp.int32)
            pl.semaphore_wait(present.at[index], count)

    settle(load_sem.at[0], 3 * 2 * DEEP * columns)
    for side in range(2):
        prepare(0, side)
    pl.semaphore_wait(barrier, expected)
    for side in range(2):
        start(to_side(0, side))
    announce(0)
    settle(load_sem.at[1], 3 * middle_rows * columns)
    start(sideways(0, TOP, rows))

    def steps(number, part, carry):
        old = arrays.at[FIELD[number]]
        for step in range(DEEP):
            last = step == DEEP - 1
            depth = step + 1
            first, count = (TOP + depth, rows - 2 * depth) if part is None else ((TOP, TOP + rows - depth)[part], depth)
            column, wide, new = 0, width, None
            if not last:
                new = work.at[step]
            else:
                column, wide = PAD, columns
                if number < ROUNDS - 1:
                    new = arrays.at[FIELD[number + 1]]

            def put(i, later, carry, new=new, column=column, wide=wide):
                if new is None:
                    density_out[i] = later
                    if carry is None:
                        return None
                    pivot, once, twice = carry
                    away = later - pivot
                    return pivot, once + away, twice + away * away
                new.reshape(tall * width, levels)[pl.ds((TOP + i) * width + column, wide), :] = later
                return carry

            if new is None and carry is None:
                advance(old, first, 1, column, wide, put, None)
                zero = jnp.zeros((columns, levels), jnp.float32)
                carry = density_out[first - TOP], zero, zero
                first, count = first + 1, count - 1
            carry = advance(old, first, count, column, wide, put, carry)
            if part is not None and not last:
                advance_beyond(part, step, old, new)
            old = new
        return carry

    hear(0)
    announce(1)
    wait_across(0)
    steps(0, None, ())
    start(sideways(1, TOP + DEEP, middle_rows))
    for side in range(2):
        wait_side(0, side)
        unpack(0, side)
        steps(0, side, ())
        prepare(1, side)
        start(to_side(1, side))
        start(sideways(1, TOP if side == 0 else TOP + rows - DEEP, DEEP))
        if side == 0:
            hear(1)
            announce(2)
    wait_across(1)
    sums = steps(1, None, None)
    for index in range(2, len(reaches)):
        hear(index)
        announce(index + 1)
    for side in range(2):
        wait_side(1, side)
        unpack(1, side)
        sums = steps(1, side, sums)
    pivot, once, twice = sums
    shift = once * (1.0 / rows)
    stats[0, 0] = pivot + shift
    stats[0, 1] = twice - once * shift
    for step in order_of(py, inner):
        do, di = step // inner, step % inner
        peer = lax.rem(my // inner + do, py // inner) * inner + lax.rem(lax.rem(my, inner) + di, inner)
        pltpu.make_async_remote_copy(
            src_ref=stats.at[0],
            dst_ref=stats.at[step],
            send_sem=stat_sem.at[0],
            recv_sem=stat_sem.at[1],
            device_id=(peer, mx),
            device_id_type=MESH,
        ).start()
    for d, (dy, dx) in enumerate(DIRECTIONS):
        @pl.when(exists(dy, dx))
        def _():
            if dy and dx:
                count = sum(CORNER)
            elif dy:
                count = parcel(0, columns) + parcel(1, columns)
            else:
                count = 10 * rows
            settle(send_sem.at[d], count)
    others = stats.at[pl.ds(1, py - 1)]
    pltpu.make_async_copy(others, others, stat_sem.at[1]).wait()
    mean = stats[0, 0]
    for step in range(1, py):
        mean = mean + stats[step, 0]
    mean = mean * (1.0 / py)
    inside = stats[0, 1]
    between = (stats[0, 0] - mean) * (stats[0, 0] - mean)
    for step in range(1, py):
        inside = inside + stats[step, 1]
        between = between + (stats[step, 0] - mean) * (stats[step, 0] - mean)
    variance = inside * (1.0 / (rows * py)) + between * (1.0 / py)
    mean_out[...] = mean
    scale_out[...] = lax.rsqrt(variance + 0.0001)
    pltpu.make_async_copy(others, others, stat_sem.at[0]).wait()

CHUNKS = 2


def finish(density, mean, scale, anomaly_out, density_out, anomaly, sem):
    rows = density.shape[0]
    whole = pltpu.make_async_copy(density, density_out, sem.at[CHUNKS])
    whole.start()
    part = rows // CHUNKS
    copies = []
    for chunk in range(CHUNKS):
        for i in range(chunk * part, (chunk + 1) * part):
            anomaly[i] = (density[i] - mean[...]) * scale[...]
        own = pl.ds(chunk * part, part)
        copies.append(pltpu.make_async_copy(anomaly.at[own], anomaly_out.at[own], sem.at[chunk]))
        copies[-1].start()
    for copy in copies:
        copy.wait()
    whole.wait()


def per_device(py, px, inner, density, conductance, source):
    rows, columns, levels = density.shape
    tall, width = rows + 2 * TOP, columns + 2 * PAD
    vmem = pl.BlockSpec(memory_space=pltpu.VMEM)
    line = jax.ShapeDtypeStruct((columns, levels), jnp.float32)
    density, conductance, source = (pltpu.with_memory_space_constraint(x, pltpu.HBM) for x in (density, conductance, source))
    density, mean, scale = pl.pallas_call(
        functools.partial(kernel, py, px, inner),
        out_shape=[jax.ShapeDtypeStruct(density.shape, jnp.float32), line, line],
        in_specs=[pl.BlockSpec(memory_space=pltpu.HBM)] * 3,
        out_specs=[vmem] * 3,
        scratch_shapes=[
            pltpu.VMEM((4, tall, width, levels), jnp.float32),
            pltpu.VMEM((DEEP - 1, tall, width, levels), jnp.float32),
            pltpu.VMEM((2, 2, width, levels), jnp.float32),
            pltpu.VMEM((ROUNDS, 2, 4 * columns + 8, levels), jnp.float32),
            pltpu.VMEM((ROUNDS, 2, 4 * columns + 8, levels), jnp.float32),
            pltpu.VMEM((ROUNDS, 2, 2, 8, levels), jnp.float32),
            pltpu.VMEM((ROUNDS, 2, 2, 8, levels), jnp.float32),
            pltpu.VMEM((py, 2, columns, levels), jnp.float32),
            pltpu.SemaphoreType.DMA((2,)),
            pltpu.SemaphoreType.DMA((len(DIRECTIONS),)),
            pltpu.SemaphoreType.DMA((ROUNDS, 2, 3)),
            pltpu.SemaphoreType.DMA((ROUNDS, 2)),
            pltpu.SemaphoreType.DMA((2,)),
            pltpu.SemaphoreType.REGULAR((max(1, len(reaches_of(py))),)),
        ],
        compiler_params=pltpu.CompilerParams(collective_id=0, has_side_effects=True, vmem_limit_bytes=10*2**20),
    )(density, conductance, source)
    return pl.pallas_call(
        finish,
        out_shape=[jax.ShapeDtypeStruct(density.shape, jnp.float32)] * 2,
        in_specs=[vmem] * 3,
        out_specs=[pl.BlockSpec(memory_space=pltpu.HBM)] * 2,
        scratch_shapes=[pltpu.VMEM(density.shape, jnp.float32), pltpu.SemaphoreType.DMA((CHUNKS + 1,))],
        compiler_params=pltpu.CompilerParams(vmem_limit_bytes=4 * 2**20),
    )(density, mean, scale)


def solution(mesh):
    spec = P("py", "px", None)
    line = mesh.devices.reshape(mesh.shape["py"], -1)[:, 0] if mesh.axis_names[0] == "py" else []
    places = [getattr(device, "coords", (0, 0, 0))[2] for device in line]
    inner = max(1, places.count(places[0])) if places else 1
    return jax.shard_map(
        functools.partial(per_device, mesh.shape["py"], mesh.shape["px"], inner),
        mesh=mesh, in_specs=(spec,) * 3, out_specs=(spec,) * 2, check_vma=False,
    )
```
